32 devices in a mesh: replica: 2 (over y), expert: 8 (over z, core), tensor: 2 (over x).
Axes of the slice: x: 2, y: 2, z: 4, core: 2. Of those that a mesh axis runs over, the one named last changes fastest.
Arguments:
- delta: bfloat16 [2, 128, 4, 14336], P('replica', 'expert', None, 'tensor'), may hold values from -6 to 6
- step_offsets: int32 [2], replicated, may hold values from 0 to 15, as said below
- block_map: int32 [128], replicated, may hold values from 0 to 127, as said below
- master_params: float32 [128, 4, 14336], P('expert', 'replica', 'tensor'), may hold values from -6 to 6
- first_moment: float32 [128, 4, 14336], P('expert', 'replica', 'tensor'), may hold values from -2 to 2
- second_moment: float32 [128, 4, 14336], P('expert', 'replica', 'tensor'), may hold values from 0.01 to 1
Outputs:
- new_params: bfloat16 [128, 4, 14336], P('expert', 'replica')
- new_first: float32 [128, 4, 14336], P('expert', 'replica', 'tensor')
- new_second: float32 [128, 4, 14336], P('expert', 'replica', 'tensor')
The draws below stay inside these ranges and needn't reach their ends.
Inputs may be any that keep to these rules, and one draw needn't show every extreme that they name: `block_map`: A permutation of the block indices onto owner slots; slot s belongs to expert index s // 16, and the blocks b with b // 16 = i go in equal numbers to every expert index. `step_offsets`: the replica groups' offsets are distinct.
All inputs are finite; a program needn't handle non-finite values.
Results may differ from the reference program's by a relative error of at most 0.0035.
Values may be sent and summed in bfloat16 or wider, within the bound.
No kernel may reach another device: no remote copies, remote signals or barrier semaphores. Data moves between devices by JAX's collectives and lax.ppermute only.
A program may use at most 64 MiB of HBM per device.

```python
import math
import jax
import jax.numpy as jnp
from jax import lax

FF = 14336
BLK_DEV = 16
BR = 4
BLOCKS = 128
REPLICAS = 2


def shuffled(key_one):
    return jax.random.permutation(key_one, BLK_DEV)


def draw_block_map(key, part):
    owners = BLOCKS // BLK_DEV
    first_key = jax.random.fold_in(key, 11)
    second_key = jax.random.fold_in(key, 23)
    source_perm = jax.vmap(shuffled)(jax.random.split(first_key, owners)).astype(jnp.int32)
    target = source_perm % owners
    ordinal = source_perm // owners
    sources = jnp.arange(owners, dtype=jnp.int32)[:, None]
    arrival = sources * (BLK_DEV // owners) + ordinal
    owner_perm = jax.vmap(shuffled)(jax.random.split(second_key, owners)).astype(jnp.int32)
    slot_ids = owner_perm[target, arrival]
    return (target * BLK_DEV + slot_ids).reshape(BLOCKS).astype(jnp.int32)


def draw_step_offsets(key, part):
    inner_key = jax.random.fold_in(key, 37)
    order_key = jax.random.fold_in(key, 41)
    middle = jax.random.permutation(inner_key, jnp.arange(1, 15, dtype=jnp.int32))[:REPLICAS - 2]
    ends = jnp.array([0, 15], dtype=jnp.int32)
    values = jnp.concatenate([ends, middle.astype(jnp.int32)])
    return jax.random.permutation(order_key, values).astype(jnp.int32)


def spiked(drawn, stream_key, source, target, blocks, factor):
    owner, partner = [(jnp.arange(drawn.shape[position]) // (drawn.shape[position] // blocks)).reshape([-1 if axis == position else 1 for axis in range(drawn.ndim)]) for position in (source, target)]
    chosen = jax.random.permutation(stream_key, blocks)[partner]
    strong = (owner == chosen) | (owner == (partner + blocks // 2) % blocks)
    return jnp.where(strong, factor * drawn, drawn)


def shard_levels(own_key, shape, shards, low, high):
    factor_of = 1.0
    for axis_at, parts in shards:
        heights = jax.random.uniform(jax.random.fold_in(jax.random.fold_in(own_key, 6), axis_at), (parts,), jnp.float32, low / len(shards), high / len(shards))
        factor_of = factor_of * jnp.repeat(jnp.exp(heights), shape[axis_at] // parts).reshape((-1,) + (1,) * (len(shape) - 1 - axis_at))
    return factor_of


def noise(own_key, dims, scale, most, pieces=(), held_as=jnp.bfloat16):
    level = shard_levels(own_key, dims, pieces, -0.22, 0.18) if pieces else 1.0
    drawn = jax.random.normal(own_key, dims, jnp.float32) * scale * level
    return jnp.minimum(jnp.maximum(drawn, -most), most).astype(held_as)


def bell_draw_with(own_key, extent, width, limit, shards, heavy, held_as=jnp.bfloat16):
    values = width * jax.random.normal(own_key, extent, jnp.float32)
    if shards:
        values = values * shard_levels(own_key, extent, shards, -0.22, 0.18)
    return jnp.clip(spiked(values, jax.random.fold_in(own_key, 3), *heavy), -limit, limit).astype(held_as)


def setup_inputs(seed: int = 0) -> dict:
    key_list = jax.random.split(jax.random.key(seed), 7)
    return {
        "delta": bell_draw_with(key_list[0], (REPLICAS, BLOCKS, BR, FF), 1.0, 6.0, ((0, 2), (1, 8), (3, 2)), (0, 2, 2, 2.0)),
        "step_offsets": draw_step_offsets(jax.random.fold_in(key_list[6], 71), 0),
        "block_map": draw_block_map(jax.random.fold_in(key_list[6], 71), 0),
        "master_params": noise(key_list[3], (BLOCKS, BR, FF), 1.0, 6.0, ((0, 8), (1, 2), (2, 2)), jnp.float32),
        "first_moment": noise(key_list[4], (BLOCKS, BR, FF), 0.3, 2.0, ((0, 8), (1, 2), (2, 2)), jnp.float32),
        "second_moment": jnp.clip(jnp.exp(math.log(1.0) - 4.6051702 * jax.random.uniform(key_list[5], (BLOCKS, BR, FF), jnp.float32) ** shard_levels(key_list[5], (BLOCKS, BR, FF), ((0, 8), (1, 2), (2, 2)), -0.2, 0.2)), 0.01, 1.0),
    }


beta_one = 0.9
beta_two = 0.99
outer_rate = 0.7
outer_round = 20
epsilon = 1e-08

def replica_weights(step_offsets):
    reciprocal = 1.0 / (1.0 + step_offsets.astype(jnp.float32))
    return reciprocal / jnp.sum(reciprocal)

def adam_update(gradient, master_params, first_moment, second_moment):
    new_first = beta_one * first_moment + (1.0 - beta_one) * gradient
    new_second = beta_two * second_moment + (1.0 - beta_two) * gradient * gradient
    fix_one = 1.0 - beta_one ** outer_round
    fix_two = 1.0 - beta_two ** outer_round
    update_step = new_first / fix_one / (jnp.sqrt(new_second / fix_two) + epsilon)
    new_params = (master_params - outer_rate * update_step).astype(jnp.bfloat16)
    return (new_params, new_first, new_second)

def reference(delta, step_offsets, block_map, master_params, first_moment, second_moment):
    weights = replica_weights(step_offsets)

    def add_replica(replica_id, running):
        slice_rows = lax.dynamic_index_in_dim(delta, replica_id, 0, keepdims=False).astype(jnp.float32)
        scaled = (slice_rows * weights[replica_id]).astype(jnp.bfloat16)
        scaled = lax.optimization_barrier(scaled)
        return running + scaled.astype(jnp.float32)
    pseudo = lax.fori_loop(0, REPLICAS, add_replica, jnp.zeros(delta.shape[1:], jnp.float32))
    inverse = jnp.argsort(block_map).astype(jnp.int32)
    gradient = pseudo[inverse]
    new_params, new_first, new_second = adam_update(gradient, master_params, first_moment, second_moment)
    return (new_params, new_first, new_second)
```

```python
import functools
import jax
import jax.numpy as jnp
from jax import lax
from jax.experimental import pallas as pl
from jax.experimental.pallas import tpu as pltpu
from jax.sharding import PartitionSpec as P

beta_one = 0.9
beta_two = 0.99
outer_rate = 0.7
outer_round = 20
epsilon = 1e-08
CHUNKS = 2
LANES = 128
FLOPS = 10**10

ANY = pl.BlockSpec(memory_space=pl.ANY)
SMEM = pl.BlockSpec(memory_space=pltpu.SMEM)
VMEM = pl.BlockSpec(memory_space=pltpu.VMEM)


def adam_update(gradient, master_params, first_moment, second_moment):
    new_first = beta_one * first_moment + (1.0 - beta_one) * gradient
    new_second = beta_two * second_moment + (1.0 - beta_two) * gradient * gradient
    fix_one = 1.0 - beta_one**outer_round
    fix_two = 1.0 - beta_two**outer_round
    update_step = new_first / fix_one / (jnp.sqrt(new_second / fix_two) + epsilon)
    new_params = (master_params - outer_rate * update_step).astype(jnp.bfloat16)
    return (new_params, new_first, new_second)


def shift_pairs(count, shift):
    return [(i, (i + shift) % count) for i in range(count)]


def column_spans(columns, chunks):
    tiles = columns // LANES
    edges = [tiles * i // chunks * LANES for i in range(chunks + 1)]
    return [(a, b) for a, b in zip(edges[:-1], edges[1:]) if b > a]


def fill_send_order(block_map, order, counts, blocks, experts):
    base = lax.axis_index("expert") * blocks
    share = blocks // experts

    def clear(d, carry):
        counts[d] = 0
        return carry

    def place(i, carry):
        owner = block_map[base + i] // blocks
        seen = counts[owner]
        order[owner * share + seen] = i
        counts[owner] = seen + 1
        return carry

    lax.fori_loop(0, experts, clear, 0)
    lax.fori_loop(0, blocks, place, 0, unroll=4)


def fill_slot_sources(block_map, sources, blocks):
    base = lax.axis_index("expert") * blocks

    def place(b, seen):
        slot = block_map[b] - base
        mine = (slot >= 0) & (slot < blocks)
        sources[jnp.where(mine, slot, blocks)] = seen
        return seen + mine.astype(jnp.int32)

    lax.fori_loop(0, block_map.shape[0], place, jnp.int32(0), unroll=8)


def replica_weight(step_offsets, replica):
    reciprocals = [
        1.0 / (1.0 + jnp.full((1, LANES), step_offsets[q], jnp.int32).astype(jnp.float32))
        for q in range(step_offsets.shape[0])
    ]
    own = reciprocals[0]
    total = reciprocals[0]
    for q in range(1, len(reciprocals)):
        own = jnp.where(replica == q, reciprocals[q], own)
        total = total + reciprocals[q]
    return (own / total)[0:1, 0:1]


def pick_rows(block, target, rows):
    picked = block[0:rows]
    for q in range(1, block.shape[0] // rows):
        picked = jnp.where(target == q, block[q * rows : (q + 1) * rows], picked)
    return picked


def weigh_kernel(block_map, step_offsets, delta, *rest, span, experts, replicas, shift):
    received, (out, local, order, counts, sem) = rest[:-5], rest[-5:]
    blocks, rows, _ = out.shape
    copy = pltpu.make_async_copy(delta.at[0, :, :, span[0] : span[1]], local, sem)
    copy.start()
    fill_send_order(block_map, order, counts, blocks, experts)
    replica = lax.axis_index("replica")
    weight = replica_weight(step_offsets, replica)
    target = lax.rem(replica + shift, replicas)
    copy.wait()

    def step(k, carry):
        block = local[order[k]].astype(jnp.float32)
        term = (pick_rows(block, target, rows) * weight).astype(jnp.bfloat16)
        if received:
            total = term.astype(jnp.float32)
            for other in received:
                total = total + other[k].astype(jnp.float32)
            term = total.astype(jnp.bfloat16)
        out[k] = term
        return carry

    lax.fori_loop(0, blocks, step, 0)


def weigh(block_map, step_offsets, delta, received, rows, span, experts, replicas, shift):
    _, blocks, all_rows, _ = delta.shape
    width = span[1] - span[0]
    return pl.pallas_call(
        functools.partial(
            weigh_kernel, span=span, experts=experts, replicas=replicas, shift=shift
        ),
        out_shape=jax.ShapeDtypeStruct((blocks, rows, width), jnp.bfloat16),
        in_specs=[SMEM, SMEM, ANY] + [VMEM] * len(received),
        out_specs=VMEM,
        scratch_shapes=[
            pltpu.VMEM((blocks, all_rows, width), delta.dtype),
            pltpu.SMEM((blocks,), jnp.int32),
            pltpu.SMEM((experts,), jnp.int32),
            pltpu.SemaphoreType.DMA,
        ],
        cost_estimate=pl.CostEstimate(flops=FLOPS, bytes_accessed=0, transcendentals=0),
        name="reduce" if received else "weigh",
    )(block_map, step_offsets, delta, *received)


def adam_kernel(block_map, grad, master, first, second, *rest, span, aliased):
    rest = rest[3:] if aliased else rest
    full, out_first, out_second, mine, states, news, sources, in_sems, out_sems = rest
    blocks = master.shape[0]
    columns = master.shape[2]
    window = pl.ds(span[0], span[1] - span[0])
    loads = [
        pltpu.make_async_copy(ref.at[:, :, window], states.at[i], in_sems.at[i])
        for i, ref in enumerate((master, first, second))
    ]
    for copy in loads:
        copy.start()
    fill_slot_sources(block_map, sources, blocks)
    for copy in loads:
        copy.wait()

    def step(s, carry):
        gradient = grad[sources[s]].astype(jnp.float32)
        mine[s], news[0, s], news[1, s] = adam_update(
            gradient, states[0, s], states[1, s], states[2, s]
        )
        return carry

    lax.fori_loop(0, blocks, step, 0)
    start = pl.multiple_of(lax.axis_index("tensor") * columns + span[0], LANES)
    stores = [
        pltpu.make_async_copy(news.at[0], out_first.at[:, :, window], out_sems.at[0]),
        pltpu.make_async_copy(news.at[1], out_second.at[:, :, window], out_sems.at[1]),
        pltpu.make_async_copy(
            mine, full.at[:, :, pl.ds(start, span[1] - span[0])], out_sems.at[2]
        ),
    ]
    for copy in stores:
        copy.start()
    for copy in stores:
        copy.wait()


def adam(block_map, grad, master, first, second, previous, span, tensors):
    blocks, rows, columns = master.shape
    width = span[1] - span[0]
    f32 = jax.ShapeDtypeStruct(master.shape, jnp.float32)
    return pl.pallas_call(
        functools.partial(adam_kernel, span=span, aliased=bool(previous)),
        out_shape=(
            jax.ShapeDtypeStruct((blocks, rows, columns * tensors), jnp.bfloat16),
            f32,
            f32,
            jax.ShapeDtypeStruct((blocks, rows, width), jnp.bfloat16),
        ),
        in_specs=[SMEM, VMEM, ANY, ANY, ANY] + [ANY] * len(previous),
        out_specs=(ANY, ANY, ANY, VMEM),
        scratch_shapes=[
            pltpu.VMEM((3, blocks, rows, width), jnp.float32),
            pltpu.VMEM((2, blocks, rows, width), jnp.float32),
            pltpu.SMEM((blocks + 1,), jnp.int32),
            pltpu.SemaphoreType.DMA((3,)),
            pltpu.SemaphoreType.DMA((3,)),
        ],
        input_output_aliases={5 + i: i for i in range(len(previous))},
        cost_estimate=pl.CostEstimate(flops=FLOPS, bytes_accessed=0, transcendentals=0),
        name="adam",
    )(block_map, grad, master, first, second, *previous)


def join_kernel(*refs, places, tensors, columns):
    pieces = refs[: len(places)]
    full, sems = refs[-2:]
    tensor = lax.axis_index("tensor")
    copies = []
    for i, (piece, (shift, start)) in enumerate(zip(pieces, places)):
        source = lax.rem(tensor + tensors - shift, tensors)
        at = pl.multiple_of(source * columns + start, LANES)
        copies.append(
            pltpu.make_async_copy(
                piece, full.at[:, :, pl.ds(at, piece.shape[2])], sems.at[i]
            )
        )
    for copy in copies:
        copy.start()
    for copy in copies:
        copy.wait()


def join(pieces, places, full, tensors):
    return pl.pallas_call(
        functools.partial(
            join_kernel, places=places, tensors=tensors, columns=full.shape[2] // tensors
        ),
        out_shape=jax.ShapeDtypeStruct(full.shape, full.dtype),
        in_specs=[VMEM] * len(pieces) + [ANY],
        out_specs=ANY,
        scratch_shapes=[pltpu.SemaphoreType.DMA((len(pieces),))],
        input_output_aliases={len(pieces): 0},
        name="join",
    )(*pieces, full)


def body(sizes, delta, step_offsets, block_map, master, first, second):
    replicas, experts, tensors = sizes
    rows, columns = master.shape[1:]
    spans = column_spans(columns, CHUNKS)
    arrived = []
    for span in spans:
        received = []
        for shift in range(1, replicas):
            sent = weigh(
                block_map, step_offsets, delta, (), rows, span, experts, replicas, shift
            )
            received.append(lax.ppermute(sent, "replica", shift_pairs(replicas, shift)))
        partial_sum = weigh(
            block_map, step_offsets, delta, tuple(received), rows, span, experts, replicas, 0
        )
        arrived.append(
            lax.all_to_all(partial_sum, "expert", split_axis=0, concat_axis=0, tiled=True)
        )
    outs = ()
    pieces = []
    places = []
    for span, grad in zip(spans, arrived):
        *outs, mine = adam(block_map, grad, master, first, second, outs, span, tensors)
        for shift in range(1, tensors):
            pieces.append(lax.ppermute(mine, "tensor", shift_pairs(tensors, shift)))
            places.append((shift, span[0]))
    full, new_first, new_second = outs
    if pieces:
        full = join(pieces, tuple(places), full, tensors)
    return (full, new_first, new_second)


def solution(mesh):
    sizes = (mesh.shape["replica"], mesh.shape["expert"], mesh.shape["tensor"])
    in_specs = (
        P("replica", "expert", None, "tensor"),
        P(),
        P(),
        P("expert", "replica", "tensor"),
        P("expert", "replica", "tensor"),
        P("expert", "replica", "tensor"),
    )
    out_specs = (
        P("expert", "replica", None),
        P("expert", "replica", "tensor"),
        P("expert", "replica", "tensor"),
    )
    return jax.shard_map(
        functools.partial(body, sizes),
        mesh=mesh,
        in_specs=in_specs,
        out_specs=out_specs,
        check_vma=False,
    )
```
